16 devices in a mesh: rep: 4 (over y, z, core), dp: 4 (over x).
Axes of the slice: x: 4, y: 2, z: 1, core: 2. Of those that a mesh axis runs over, the one named last changes fastest.
The devices are a block of a 4x4x8 slice.
Arguments:
- x: bfloat16 [16, 4096, 512], P(('rep', 'dp')), parts along dimension 0
- dy: bfloat16 [16, 4096, 512], P(('rep', 'dp')), parts along dimension 0
- w_gate: bfloat16 [2, 512, 1664], replicated
- w_up: bfloat16 [2, 512, 1664], replicated
- w_down: bfloat16 [2, 1664, 512], replicated
- m_w_gate: float32 [2, 512, 1664], replicated
- m_w_up: float32 [2, 512, 1664], replicated
- m_w_down: float32 [2, 1664, 512], replicated
- v_w_gate: float32 [2, 512, 1664], replicated
- v_w_up: float32 [2, 512, 1664], replicated
- v_w_down: float32 [2, 1664, 512], replicated
Outputs:
- output 1: bfloat16 [8, 512, 1664], P('rep'), parts along dimension 0
- output 2: bfloat16 [8, 512, 1664], P('rep'), parts along dimension 0
- output 3: bfloat16 [8, 1664, 512], P('rep'), parts along dimension 0
- output 4: float32 [8, 512, 1664], P('rep'), parts along dimension 0
- output 5: float32 [8, 512, 1664], P('rep'), parts along dimension 0
- output 6: float32 [8, 1664, 512], P('rep'), parts along dimension 0
- output 7: float32 [8, 512, 1664], P('rep'), parts along dimension 0
- output 8: float32 [8, 512, 1664], P('rep'), parts along dimension 0
- output 9: float32 [8, 1664, 512], P('rep'), parts along dimension 0
There are 4 independent parts. The reference program is written for one: setup_inputs(seed, part) draws one part's arguments, and reference() takes and returns one part's arrays. A program takes and returns all parts, laid end to end along the dimension named above; an argument that names none is the same for every part.
All inputs are finite; a program needn't handle non-finite values.
Results may differ from the reference program's by a relative error of at most 0.022.
Values are sent between devices in bfloat16 or wider.
A program may use at most 768 MiB of HBM per device.

```python
import jax
import jax.numpy as jnp
from jax import lax

SEQUENCES = 4
TOKENS = 4096
D = 512
FF = 1664
LAYERS = 2
NAMES = ("w_gate", "w_up", "w_down")
SHAPES = {"w_gate": (LAYERS, D, FF), "w_up": (LAYERS, D, FF), "w_down": (LAYERS, FF, D)}


def bump(key, n, height):
    away = (jnp.arange(n, dtype=jnp.int32) - jax.random.randint(key, (), 0, n, jnp.int32)) % n
    return jnp.where(away < n // 8, height, 1.0)


def together(key, own, strength):
    shared = jax.random.normal(key, own.shape[1:], jnp.float32)
    return (own + strength * shared) * lax.rsqrt(1 + strength * strength)


def setup_inputs(seed: int = 0, part: int = 0) -> dict:
    kx, kdy, ka, kb, kz, kf, kh, kl, *keys = jax.random.split(jax.random.key(seed), 8 + 3 * len(NAMES))
    kx, kdy, ka, kb = (jax.random.fold_in(k, part) for k in (kx, kdy, ka, kb))
    kw, km, kv = (keys[i::3] for i in range(3))
    shape = (SEQUENCES, TOKENS, D)
    much_x, much_dy = jax.random.uniform(kz, (2,), jnp.float32, 0.0, 1.0)
    loud = 2.0 ** jax.random.uniform(jax.random.fold_in(kz, 1), (), jnp.float32, -1.0, 2.0)
    layers = 2.0 ** jax.random.uniform(kl, (LAYERS, 1, 1), jnp.float32, -1.0, 1.0)
    x = together(ka, jax.random.normal(kx, shape, jnp.float32), much_x) * bump(kf, D, 4.0)
    dy = together(kb, jax.random.normal(kdy, shape, jnp.float32), much_dy)
    drawn = {"x": x.astype(jnp.bfloat16), "dy": (loud * dy * (SEQUENCES * TOKENS) ** -0.5).astype(jnp.bfloat16)}
    for key, name in zip(kw, NAMES, strict=True):
        w = jax.random.normal(key, SHAPES[name], jnp.float32) * SHAPES[name][1] ** -0.5
        drawn[name] = (w * {"w_gate": 1.0, "w_up": bump(kh, FF, 4.0), "w_down": layers}[name]).astype(jnp.bfloat16)
    for key, name in zip(km, NAMES, strict=True):
        drawn[f"m_{name}"] = 0.1 * jax.random.normal(key, SHAPES[name], jnp.float32)
    for key, name in zip(kv, NAMES, strict=True):
        drawn[f"v_{name}"] = jax.random.uniform(key, SHAPES[name], jnp.float32, 0.005, 0.015)
    return drawn


def matmul(a, w):
    return jnp.dot(a, w, preferred_element_type=jnp.float32).astype(jnp.bfloat16)


def normed(h):
    wide = h.astype(jnp.float32)
    scale = lax.rsqrt(jnp.mean(wide**2, -1, keepdims=True) + 1e-6)
    return (wide * scale).astype(jnp.bfloat16)


def layer(h, w):
    a = normed(h)
    gate = jnp.dot(a, w["w_gate"], preferred_element_type=jnp.float32)
    up = jnp.dot(a, w["w_up"], preferred_element_type=jnp.float32)
    return h + matmul((jax.nn.silu(gate) * up).astype(jnp.bfloat16), w["w_down"])


def adamw(w, m, v, g):
    m = 0.9 * m + 0.1 * g
    v = 0.95 * v + 0.05 * g * g
    step = m * lax.rsqrt(v + 1e-8) + 0.1 * w
    return (w - 0.02 * step).astype(jnp.bfloat16), m, v


def clipped(gradients, sum_of_squares, count):
    factor = jnp.minimum(1.0, 0.5 * lax.rsqrt(sum_of_squares / count + 1e-30))
    return [g * factor for g in gradients]


def stack(weights, h):
    return lax.scan(lambda h, w: (layer(h, w), None), h, weights)[0]


def reference(x, dy, w_gate, w_up, w_down, m_w_gate, m_w_up, m_w_down, v_w_gate, v_w_up, v_w_down):
    weights = dict(zip(NAMES, (w_gate, w_up, w_down), strict=True))

    def take(so_far, sequence):
        h, by_y = sequence
        _, back = jax.vjp(lambda w: stack(w, h), weights)
        return jax.tree.map(lambda total, term: total + term.astype(jnp.float32), so_far, back(by_y)[0]), None

    none_yet = {name: jnp.zeros(w.shape, jnp.float32) for name, w in weights.items()}
    by_weights, _ = lax.scan(take, none_yet, (x, dy))
    gradients = [by_weights[name].astype(jnp.bfloat16).astype(jnp.float32) for name in NAMES]
    gradients = clipped(gradients, sum(jnp.sum(g * g) for g in gradients), sum(g.size for g in gradients))
    new = [
        adamw(w.astype(jnp.float32), m, v, g)
        for w, m, v, g in zip((w_gate, w_up, w_down), (m_w_gate, m_w_up, m_w_down), (v_w_gate, v_w_up, v_w_down), gradients, strict=True)
    ]
    return tuple(one[which] for which in range(3) for one in new)
```

```python
import functools

import jax
import jax.numpy as jnp
from jax import lax
from jax.experimental import pallas as pl
from jax.experimental.pallas import tpu as pltpu
from jax.sharding import PartitionSpec as P

F32, BF16 = jnp.float32, jnp.bfloat16
MESH = pl.DeviceIdType.MESH
LANES = 128
VMEM_LIMIT = 67043328
TILE = 512
CHUNK = 2 * LANES


def by_columns(a, b):
    return lax.dot_general(a, b, (((1,), (1,)), ((), ())), preferred_element_type=F32)


def tokens_kernel(x_ref, dy_ref, wg_ref, wu_ref, wd_ref, dyt_ref, a1t_ref, dht_ref, a0t_ref, hid1_ref, dgu1_ref, hid0_ref, dgu0_ref,
                  wgu, wd, keep, sems, *, many):
    layers, ff, _ = wd.shape
    blocks = ff // LANES

    @pl.when(pl.program_id(0) == 0)
    def _():
        copies = []
        for n in range(layers):
            for k in range(blocks):
                for which, ref in enumerate((wg_ref, wu_ref)):
                    at = 2 * k + which
                    copies.append(pltpu.make_async_copy(
                        ref.at[n, :, pl.ds(k * LANES, LANES)], wgu.at[n, :, pl.ds(at * LANES, LANES)], sems.at[n, at]))
            copies.append(pltpu.make_async_copy(wd_ref.at[n], wd.at[n], sems.at[n, 2 * blocks]))
        for copy in copies:
            copy.start()
        for copy in copies:
            copy.wait()

    def scaled(h):
        wide = h.astype(F32)
        scale = lax.rsqrt(jnp.mean(wide * wide, -1, keepdims=True) + 1e-6)
        return wide, scale, (wide * scale).astype(BF16)

    def lane(k):
        return pl.ds(k * LANES, LANES)

    groups = [(k, min(many, blocks - k)) for k in range(0, blocks, many)]
    h0 = x_ref[...]
    _, _, a0 = scaled(h0)
    a0t_ref[...] = a0.T
    for k, count in groups:
        gu = jnp.dot(a0, wgu[0, :, pl.ds(2 * k * LANES, 2 * count * LANES)], preferred_element_type=F32)
        for i in range(count):
            g, u = (gu[:, (2 * i + j) * LANES : (2 * i + j + 1) * LANES] for j in range(2))
            s = 0.5 * jnp.tanh(0.5 * g) + 0.5
            silu = g * s
            hid0_ref[:, lane(k + i)] = (silu * u).astype(BF16)
            keep[:, lane(2 * (k + i))] = (s + silu * (1.0 - s)) * u
            keep[:, lane(2 * (k + i) + 1)] = silu
    h1 = h0 + jnp.dot(hid0_ref[...], wd[0], preferred_element_type=F32).astype(BF16)
    wide, scale, a1 = scaled(h1)
    a1t_ref[...] = a1.T
    dy = dy_ref[...]
    dyt_ref[...] = dy.T
    for k, count in groups:
        gu = jnp.dot(a1, wgu[1, :, pl.ds(2 * k * LANES, 2 * count * LANES)], preferred_element_type=F32)
        dhid = by_columns(dy, wd[1, pl.ds(k * LANES, count * LANES), :]).astype(BF16).astype(F32)
        for i in range(count):
            g, u = (gu[:, (2 * i + j) * LANES : (2 * i + j + 1) * LANES] for j in range(2))
            dh = dhid[:, i * LANES : (i + 1) * LANES]
            s = 0.5 * jnp.tanh(0.5 * g) + 0.5
            silu = g * s
            hid1_ref[:, lane(k + i)] = (silu * u).astype(BF16)
            dgu1_ref[:, lane(2 * (k + i))] = (dh * u * (s + silu * (1.0 - s))).astype(BF16)
            dgu1_ref[:, lane(2 * (k + i) + 1)] = (dh * silu).astype(BF16)
    da = by_columns(dgu1_ref[...], wgu[1]).astype(BF16).astype(F32)
    along = jnp.mean(da * wide, -1, keepdims=True)
    dh1 = dy + (scale * (da - wide * (scale * scale) * along)).astype(BF16)
    dht_ref[...] = dh1.T
    for k, count in groups:
        dhid = by_columns(dh1, wd[0, pl.ds(k * LANES, count * LANES), :]).astype(BF16).astype(F32)
        for i in range(count):
            dh = dhid[:, i * LANES : (i + 1) * LANES]
            for j in range(2):
                at = lane(2 * (k + i) + j)
                dgu0_ref[:, at] = (dh * keep[:, at]).astype(BF16)


def tokens_pass(x, dy, wg, wu, wd):
    _, tokens, d = x.shape
    layers, ff, _ = wd.shape
    tile = min(TILE, tokens)
    lead = pl.BlockSpec((None, tile, d), lambda i: (0, i, 0))
    hbm = pl.BlockSpec(memory_space=pl.ANY)
    turned = pl.BlockSpec((d, tile), lambda i: (0, i))
    widths = (ff, 2 * ff, ff, 2 * ff)
    return pl.pallas_call(
        functools.partial(tokens_kernel, many=2),
        grid=(tokens // tile,),
        out_shape=[jax.ShapeDtypeStruct((d, tokens), BF16)] * 4 + [jax.ShapeDtypeStruct((tokens, n), BF16) for n in widths],
        in_specs=[lead, lead, hbm, hbm, hbm],
        out_specs=[turned] * 4 + [pl.BlockSpec((tile, n), lambda i: (i, 0)) for n in widths],
        scratch_shapes=[
            pltpu.VMEM((layers, d, 2 * ff), BF16),
            pltpu.VMEM((layers, ff, d), BF16),
            pltpu.VMEM((tile, 2 * ff), F32),
            pltpu.SemaphoreType.DMA((layers, 2 * ff // LANES + 1)),
        ],
        compiler_params=pltpu.CompilerParams(vmem_limit_bytes=VMEM_LIMIT, dimension_semantics=("arbitrary",)),
        cost_estimate=pl.CostEstimate(flops=2 * 9 * tokens * d * ff, bytes_accessed=16 * tokens * ff, transcendentals=2 * tokens * ff),
        name="tokens",
    )(x, dy, wg, wu, wd)


(VIA_LEFT, VIA_RIGHT, OWN_LEFT, OWN_RIGHT, SUM_LEFT, SUM_RIGHT, ALL_LEFT, ALL_RIGHT, FAR_LEFT, FAR_RIGHT) = range(10)


def units_of(layers, ff):
    cut = (ff // LANES // 2) * LANES
    return [(down, n, start, size) for n in reversed(range(layers)) for down in (True, False) for start, size in ((0, cut), (cut, ff - cut))]


def reduce_kernel(n, dyt_ref, a1t_ref, dht_ref, a0t_ref, hid1_ref, dgu1_ref, hid0_ref, dgu0_ref, gd_out, gg_out, gu_out, sq_out,
                  lefts, rights, own_d, own_gu, via_d, via_gu, in_d, in_gu, all_d, all_gu, squares,
                  left_sem, right_sem, send, recv, sq_send, sq_recv, out_sem):
    layers, ff, d = own_d.shape
    units = units_of(layers, ff)
    me = lax.axis_index("dp")
    right, left, far = lax.rem(me + 1, n), lax.rem(me + n - 1, n), lax.rem(me + n // 2, n)

    barrier = pltpu.get_barrier_semaphore()
    for step in range(1, n):
        pl.semaphore_signal(barrier, inc=1, device_id={"dp": lax.rem(me + step, n)}, device_id_type=MESH)

    def share(ref, unit, owner, half):
        down, layer, start, size = unit
        rows = (size if down else d) // n
        first = owner * rows
        if half is not None:
            rows = rows // 2
            first = first + half * rows
        if down:
            return ref[0].at[layer, pl.ds(pl.multiple_of(start + first, 16), rows), :]
        return ref[1].at[layer, :, pl.ds(pl.multiple_of(first, 16), rows), pl.ds(start, size)]

    def slot(ref, unit, k):
        down, layer, start, size = unit
        if down:
            return ref[0].at[k, layer, pl.ds(start // (2 * n), size // (2 * n)), :]
        return ref[1].at[k, layer, :, :, pl.ds(start, size)]

    own, via, arrived, whole = (own_d, own_gu), (via_d, via_gu), (in_d, in_gu), (all_d, all_gu)

    def remote(u, kind):
        unit = units[u]
        to = left if kind % 2 == 0 else right
        if kind in (VIA_LEFT, VIA_RIGHT):
            src, dst = share(own, unit, far, kind - VIA_LEFT), slot(via, unit, kind - VIA_LEFT)
        elif kind in (OWN_LEFT, OWN_RIGHT):
            src, dst = share(own, unit, to, 1 if kind == OWN_LEFT else 0), slot(arrived, unit, 1 if kind == OWN_LEFT else 0)
        elif kind in (SUM_LEFT, SUM_RIGHT):
            src, dst = share(own, unit, to, kind - SUM_LEFT), slot(arrived, unit, 2 + kind - SUM_LEFT)
        elif kind in (ALL_LEFT, ALL_RIGHT):
            src = dst = share(whole, unit, me, None)
        else:
            src = dst = share(whole, unit, right if kind == FAR_LEFT else left, 1 if kind == FAR_LEFT else 0)
        return pltpu.make_async_remote_copy(src_ref=src, dst_ref=dst, send_sem=send.at[u, kind], recv_sem=recv.at[u, kind],
                                            device_id={"dp": to}, device_id_type=MESH)

    def start(u, *kinds):
        for kind in kinds:
            remote(u, kind).start()

    def arrive(u, *kinds):
        for kind in kinds:
            remote(u, kind).wait_recv()

    def each(unit, body):
        down, _, _, size = unit
        blocks = (size if down else d) // (2 * n) // 16
        for which in range(1 if down else 2):
            def one(i, _, which=which):
                rows = pl.ds(pl.multiple_of(i * 16, 16), 16)
                body((rows, slice(None)) if down else (which, rows, slice(None)))
                return 0

            lax.fori_loop(0, blocks, one, 0)

    def forward_sums(u):
        unit = units[u]
        for k, kind, owner in ((0, SUM_LEFT, left), (1, SUM_RIGHT, right)):
            arrive(u, VIA_LEFT + k)
            mine, other = share(own, unit, owner, k), slot(via, unit, k)

            def add(at, mine=mine, other=other):
                mine[at] = (mine[at].astype(F32) + other[at].astype(F32)).astype(BF16)

            each(unit, add)
            start(u, kind)

    def finish(u):
        unit = units[u]
        arrive(u, OWN_LEFT, OWN_RIGHT, SUM_LEFT, SUM_RIGHT)
        for half in range(2):
            mine, out = share(own, unit, me, half), share(whole, unit, me, half)
            one, two = slot(arrived, unit, half), slot(arrived, unit, 2 + half)

            def add(at, mine=mine, out=out, one=one, two=two):
                g = (mine[at].astype(F32) + one[at].astype(F32) + two[at].astype(F32)).astype(BF16)
                out[at] = g
                wide = g.astype(F32)
                wide = wide * wide
                total = wide[:, :LANES]
                for k in range(1, wide.shape[1] // LANES):
                    total = total + wide[:, k * LANES : (k + 1) * LANES]
                squares[n] = squares[n] + total

            each(unit, add)

    firsts = {True: (dyt_ref, dht_ref), False: (a1t_ref, a0t_ref)}
    seconds = {True: (hid1_ref, hid0_ref), False: (dgu1_ref, dgu0_ref)}
    loads = []
    for k, ref in enumerate((dyt_ref, a1t_ref, dht_ref, a0t_ref)):
        loads.append(pltpu.make_async_copy(ref, lefts.at[k], left_sem.at[k]))

    def chunks(u):
        down, _, start_, size = units[u]
        scale = 1 if down else 2
        return scale * start_, scale * size, -(-scale * size // CHUNK)

    def source(u):
        down, layer, _, _ = units[u]
        return seconds[down][layers - 1 - layer]

    def fetch(u, c, parity):
        base, width, _ = chunks(u)
        first = base + jnp.minimum(c * CHUNK, width - CHUNK)
        return pltpu.make_async_copy(source(u).at[:, pl.ds(pl.multiple_of(first, LANES), CHUNK)], rights.at[parity], right_sem.at[parity])

    fetch(0, 0, 0).start()
    loads[0].start()
    for load in loads[1:]:
        load.start()

    done = 0
    for u, unit in enumerate(units):
        down, layer, begin, size = unit
        which = 2 * (layers - 1 - layer) + (0 if down else 1)
        base, width, count = chunks(u)
        if begin == 0:
            loads[which].wait()

        def one(c, _, u=u, down=down, layer=layer, which=which, base=base, width=width, count=count, done=done):
            parity = lax.rem(done + c, 2)
            fetch(u, c, parity).wait()

            @pl.when(c + 1 < count)
            def _():
                fetch(u, c + 1, 1 - parity).start()

            if u + 1 < len(units):
                @pl.when(c + 1 == count)
                def _():
                    fetch(u + 1, 0, 1 - parity).start()

            g = jnp.dot(lefts[which], rights[parity], preferred_element_type=F32).astype(BF16)
            first = base + jnp.minimum(c * CHUNK, width - CHUNK)
            if down:
                own_d[layer, pl.ds(pl.multiple_of(first, LANES), CHUNK), :] = g.T
            else:
                at = pl.ds(pl.multiple_of(first // 2, LANES), LANES)
                own_gu[layer, 0, :, at] = g[:, :LANES]
                own_gu[layer, 1, :, at] = g[:, LANES:]
            return 0

        lax.fori_loop(0, count, one, 0)
        done += count
        if u == 0:
            squares[n] = jnp.zeros(squares.shape[1:], F32)
            pl.semaphore_wait(barrier, n - 1)
        start(u, VIA_LEFT, VIA_RIGHT, OWN_LEFT, OWN_RIGHT)
        if u >= 1:
            forward_sums(u - 1)
        if u >= 2:
            finish(u - 2)
    last = len(units) - 1
    start(0, ALL_LEFT, ALL_RIGHT)
    forward_sums(last)
    finish(last - 1)
    finish(last)

    squares[me] = squares[n]
    exchange = [
        pltpu.make_async_remote_copy(src_ref=squares.at[me], dst_ref=squares.at[me], send_sem=sq_send.at[step], recv_sem=sq_recv.at[step],
                                     device_id={"dp": lax.rem(me + step, n)}, device_id_type=MESH)
        for step in range(1, n)
    ]
    for copy in exchange:
        copy.start()
    for u in range(1, len(units)):
        start(u, ALL_LEFT, ALL_RIGHT)
    for copy in exchange:
        copy.wait_recv()
    total = squares[0]
    for k in range(1, n):
        total = total + squares[k]
    sq_out[...] = total

    for u in range(len(units)):
        arrive(u, ALL_LEFT, ALL_RIGHT)
        start(u, FAR_LEFT, FAR_RIGHT)
    outs = []
    for u, (down, layer, begin, size) in enumerate(units):
        arrive(u, FAR_LEFT, FAR_RIGHT)
        at = pl.ds(begin, size)
        if down:
            outs.append(pltpu.make_async_copy(all_d.at[layer, at, :], gd_out.at[layer, at, :], out_sem.at[u, 0]))
            outs[-1].start()
        else:
            for k, out in enumerate((gg_out, gu_out)):
                outs.append(pltpu.make_async_copy(all_gu.at[layer, k, :, at], out.at[layer, :, at], out_sem.at[u, k]))
                outs[-1].start()
    for u in range(len(units)):
        for kind in range(10):
            remote(u, kind).wait_send()
    for copy in exchange:
        copy.wait_send()
    for out in outs:
        out.wait()


def reduced(n, layers, d, ff, tokens, parts):
    hbm = pl.BlockSpec(memory_space=pl.ANY)
    units = len(units_of(layers, ff))
    dma = pltpu.SemaphoreType.DMA
    return pl.pallas_call(
        functools.partial(reduce_kernel, n),
        out_shape=[
            jax.ShapeDtypeStruct((layers, ff, d), BF16),
            jax.ShapeDtypeStruct((layers, d, ff), BF16),
            jax.ShapeDtypeStruct((layers, d, ff), BF16),
            jax.ShapeDtypeStruct((16, LANES), F32),
        ],
        in_specs=[hbm] * 8,
        out_specs=[hbm] * 3 + [pl.BlockSpec(memory_space=pltpu.VMEM)],
        scratch_shapes=[
            pltpu.VMEM((4, d, tokens), BF16),
            pltpu.VMEM((2, tokens, CHUNK), BF16),
            pltpu.VMEM((layers, ff, d), BF16),
            pltpu.VMEM((layers, 2, d, ff), BF16),
            pltpu.VMEM((2, layers, ff // (2 * n), d), BF16),
            pltpu.VMEM((2, layers, 2, d // (2 * n), ff), BF16),
            pltpu.VMEM((4, layers, ff // (2 * n), d), BF16),
            pltpu.VMEM((4, layers, 2, d // (2 * n), ff), BF16),
            pltpu.VMEM((layers, ff, d), BF16),
            pltpu.VMEM((layers, 2, d, ff), BF16),
            pltpu.VMEM((n + 1, 16, LANES), F32),
            dma((4,)),
            dma((2,)),
            dma((units, 10)),
            dma((units, 10)),
            dma((n,)),
            dma((n,)),
            dma((units, 2)),
        ],
        compiler_params=pltpu.CompilerParams(vmem_limit_bytes=VMEM_LIMIT, collective_id=0, has_side_effects=True),
        cost_estimate=pl.CostEstimate(flops=2 * 6 * tokens * d * ff, bytes_accessed=16 * tokens * ff, transcendentals=0),
        name="reduce",
    )(*parts)


def adamw_kernel(count, sq_ref, *refs):
    factor = jnp.minimum(1.0, 0.5 * lax.rsqrt(jnp.sum(sq_ref[...], keepdims=True) / count + 1e-30))
    for i in range(3):
        g_ref, w_ref, m_ref, v_ref, new_w, new_m, new_v = refs[i::3]
        g = g_ref[...].astype(F32) * factor
        w = w_ref[...].astype(F32)
        m = 0.9 * m_ref[...] + 0.1 * g
        v = 0.95 * v_ref[...] + 0.05 * g * g
        step = m * lax.rsqrt(v + 1e-8) + 0.1 * w
        new_w[...] = (w - 0.02 * step).astype(BF16)
        new_m[...] = m
        new_v[...] = v


def adamw(squares, gradients, weights, m, v, steps=16):
    flat = [[a.reshape(-1, a.shape[-1]) for a in group] for group in (gradients, weights, m, v)]
    shapes = [w.shape for w in flat[1]]
    specs = [pl.BlockSpec((rows // steps, columns), lambda i: (i, 0)) for rows, columns in shapes]
    count = sum(w.size for w in weights)
    new = pl.pallas_call(
        functools.partial(adamw_kernel, count),
        grid=(steps,),
        out_shape=[jax.ShapeDtypeStruct(shape, dtype) for dtype in (BF16, F32, F32) for shape in shapes],
        in_specs=[pl.BlockSpec(squares.shape, lambda i: (0, 0))] + specs * 4,
        out_specs=specs * 3,
        compiler_params=pltpu.CompilerParams(vmem_limit_bytes=VMEM_LIMIT, dimension_semantics=("arbitrary",)),
        cost_estimate=pl.CostEstimate(flops=16 * count, bytes_accessed=22 * count, transcendentals=count),
        name="adamw",
    )(squares, *(a for group in flat for a in group))
    return tuple(a.reshape(w.shape) for a, w in zip(new, weights * 3, strict=True))


def solution(mesh):
    n = mesh.shape["dp"]

    def step(x, dy, *arrays):
        weights, m, v = (arrays[i : i + 3] for i in (0, 3, 6))
        layers, ff, d = weights[2].shape
        parts = tokens_pass(x, dy, *weights)
        gd, gg, gu, squares = reduced(n, layers, d, ff, x.shape[1], parts)
        return adamw(squares, (gg, gu, gd), weights, m, v)

    return jax.shard_map(
        step,
        mesh=mesh,
        in_specs=(P(("rep", "dp"), None, None),) * 2 + (P(None, None, None),) * 9,
        out_specs=(P("rep", None, None),) * 9,
        check_vma=False,
    )
```

```python
import functools

import jax
import jax.numpy as jnp
from jax import lax
from jax.experimental import pallas as pl
from jax.experimental.pallas import tpu as pltpu
from jax.sharding import PartitionSpec as P

F32, BF16 = jnp.float32, jnp.bfloat16
MESH = pl.DeviceIdType.MESH
LANES = 128
VMEM_LIMIT = 67043328
TILE = 512
CHUNK = 4 * LANES


def by_columns(a, b):
    return lax.dot_general(a, b, (((1,), (1,)), ((), ())), preferred_element_type=F32)


def scaled(h):
    wide = h.astype(F32)
    scale = lax.rsqrt(jnp.mean(wide * wide, -1, keepdims=True) + 1e-6)
    return wide, scale, (wide * scale).astype(BF16)


def lane(k):
    return pl.ds(k * LANES, LANES)


def side_by_side(wg_ref, wu_ref, wgu, n, sems):
    return [
        pltpu.make_async_copy(ref.at[n, :, lane(k)], wgu.at[:, lane(2 * k + which)], sems.at[2 * k + which])
        for k in range(wg_ref.shape[-1] // LANES)
        for which, ref in enumerate((wg_ref, wu_ref))
    ]


def grouped(blocks, many):
    return [(k, min(many, blocks - k)) for k in range(0, blocks, many)]


def tokens_kernel(x_ref, dy_ref, wg_ref, wu_ref, wd_ref, dyt_ref, a1t_ref, a0t_ref, h1_ref, hid1_ref, dgu1_ref, hid0_ref,
                  keep_ref, wgu, wd, sems, *, many):
    layers, ff, _ = wd.shape
    blocks = ff // LANES

    @pl.when(pl.program_id(0) == 0)
    def _():
        copies = []
        for n in range(layers):
            copies += side_by_side(wg_ref, wu_ref, wgu.at[n], n, sems.at[n])
            copies.append(pltpu.make_async_copy(wd_ref.at[n], wd.at[n], sems.at[n, 2 * blocks]))
        for copy in copies:
            copy.start()
        for copy in copies:
            copy.wait()

    groups = grouped(blocks, many)
    h0 = x_ref[...]
    _, _, a0 = scaled(h0)
    a0t_ref[...] = a0.T
    for k, count in groups:
        gu = jnp.dot(a0, wgu[0, :, pl.ds(2 * k * LANES, 2 * count * LANES)], preferred_element_type=F32)
        for i in range(count):
            g, u = (gu[:, (2 * i + j) * LANES : (2 * i + j + 1) * LANES] for j in range(2))
            s = 0.5 * jnp.tanh(0.5 * g) + 0.5
            silu = g * s
            hid0_ref[:, lane(k + i)] = (silu * u).astype(BF16)
            keep_ref[:, lane(2 * (k + i))] = (s + silu * (1.0 - s)) * u
            keep_ref[:, lane(2 * (k + i) + 1)] = silu
    h1 = h0 + jnp.dot(hid0_ref[...], wd[0], preferred_element_type=F32).astype(BF16)
    h1_ref[...] = h1
    _, _, a1 = scaled(h1)
    a1t_ref[...] = a1.T
    dy = dy_ref[...]
    dyt_ref[...] = dy.T
    for k, count in groups:
        gu = jnp.dot(a1, wgu[1, :, pl.ds(2 * k * LANES, 2 * count * LANES)], preferred_element_type=F32)
        dhid = by_columns(dy, wd[1, pl.ds(k * LANES, count * LANES), :]).astype(BF16).astype(F32)
        for i in range(count):
            g, u = (gu[:, (2 * i + j) * LANES : (2 * i + j + 1) * LANES] for j in range(2))
            dh = dhid[:, i * LANES : (i + 1) * LANES]
            s = 0.5 * jnp.tanh(0.5 * g) + 0.5
            silu = g * s
            hid1_ref[:, lane(k + i)] = (silu * u).astype(BF16)
            dgu1_ref[:, lane(2 * (k + i))] = (dh * u * (s + silu * (1.0 - s))).astype(BF16)
            dgu1_ref[:, lane(2 * (k + i) + 1)] = (dh * silu).astype(BF16)


def tokens_pass(x, dy, wg, wu, wd):
    _, tokens, d = x.shape
    layers, ff, _ = wd.shape
    tile = min(TILE, tokens)
    lead = pl.BlockSpec((None, tile, d), lambda i: (0, i, 0))
    hbm = pl.BlockSpec(memory_space=pl.ANY)
    turned = pl.BlockSpec((d, tile), lambda i: (0, i))
    widths = (d, ff, 2 * ff, ff, 2 * ff)
    return pl.pallas_call(
        functools.partial(tokens_kernel, many=2),
        grid=(tokens // tile,),
        out_shape=[jax.ShapeDtypeStruct((d, tokens), BF16)] * 3 + [
            jax.ShapeDtypeStruct((tokens, n), F32 if k == 4 else BF16) for k, n in enumerate(widths)
        ],
        in_specs=[lead, lead, hbm, hbm, hbm],
        out_specs=[turned] * 3 + [pl.BlockSpec((tile, n), lambda i: (i, 0)) for n in widths],
        scratch_shapes=[
            pltpu.VMEM((layers, d, 2 * ff), BF16),
            pltpu.VMEM((layers, ff, d), BF16),
            pltpu.SemaphoreType.DMA((layers, 2 * ff // LANES + 1)),
        ],
        compiler_params=pltpu.CompilerParams(vmem_limit_bytes=VMEM_LIMIT, dimension_semantics=("arbitrary",)),
        cost_estimate=pl.CostEstimate(flops=2 * 6 * tokens * d * ff, bytes_accessed=10 * tokens * ff, transcendentals=2 * tokens * ff),
        name="tokens",
    )(x, dy, wg, wu, wd)


(VIA_LEFT, VIA_RIGHT, OWN_LEFT, OWN_RIGHT, SUM_LEFT, SUM_RIGHT, ALL_LEFT, ALL_RIGHT, FAR_LEFT, FAR_RIGHT) = range(10)


def units_of(layers, ff):
    cuts = {True: CHUNK, False: (ff // CHUNK) * CHUNK // 2}
    return [
        (down, n, start, size)
        for n in reversed(range(layers))
        for down, cut in cuts.items()
        for start, size in ((0, cut), (cut, ff - cut))
    ]


def reduce_kernel(n, dyt_ref, a1t_ref, a0t_ref, h1_ref, hid1_ref, dgu1_ref, hid0_ref, keep_ref, dy_ref, wg_ref, wu_ref, wd_ref,
                  gd_out, gg_out, gu_out, part_a, part_b, sq_out, places, dgu0_ref,
                  lefts, rights, own_d, own_gu, via_d, via_gu, in_d, in_gu, all_d, all_gu, mine_d, mine_gu, squares,
                  wgu, wd, dgu1_in, keep_in, small_in, dgu0_tile,
                  left_sem, right_sem, send, recv, sq_send, sq_recv, out_sem, weight_sem, tile_sem, back_sem):
    layers, ff, d = own_d.shape
    tile = dgu0_tile.shape[1]
    tiles = h1_ref.shape[0] // tile
    units = units_of(layers, ff)
    me = lax.axis_index("dp")
    right, left, far = lax.rem(me + 1, n), lax.rem(me + n - 1, n), lax.rem(me + n // 2, n)

    barrier = pltpu.get_barrier_semaphore()
    for step in range(1, n):
        pl.semaphore_signal(barrier, inc=1, device_id={"dp": lax.rem(me + step, n)}, device_id_type=MESH)

    def within(unit, owner, half):
        down, _, start, size = unit
        if down:
            rows = pl.ds(start, size) if half is None else pl.ds(start + half * (size // 2), size // 2)
            return rows, pl.ds(pl.multiple_of(owner * LANES, LANES), LANES)
        rows = d // n
        first = owner * rows
        if half is not None:
            rows = rows // 2
            first = first + half * rows
        return slice(None), pl.ds(pl.multiple_of(first, 16), rows), pl.ds(start, size)

    def share(ref, unit, owner, half):
        return ref[0 if unit[0] else 1].at[(unit[1], *within(unit, owner, half))]

    def shared(unit, owner, half):
        return whole[0 if unit[0] else 1].at[within(unit, owner, half)]

    def slot(ref, unit, k):
        down, layer, start, size = unit
        if down:
            return ref[0].at[k, pl.ds(start // 2, size // 2), :]
        return ref[1].at[k, :, :, pl.ds(start, size)]

    def summed(unit, half):
        if unit[1]:
            return shared(unit, me, half)
        return (mine_d if unit[0] else mine_gu).at[within(unit, 0, half)]

    own, via, arrived, whole = (own_d, own_gu), (via_d, via_gu), (in_d, in_gu), (all_d, all_gu)

    def remote(u, kind):
        unit = units[u]
        to = left if kind % 2 == 0 else right
        if kind in (VIA_LEFT, VIA_RIGHT):
            src, dst = share(own, unit, far, kind - VIA_LEFT), slot(via, unit, kind - VIA_LEFT)
        elif kind in (OWN_LEFT, OWN_RIGHT):
            src, dst = share(own, unit, to, 1 if kind == OWN_LEFT else 0), slot(arrived, unit, 1 if kind == OWN_LEFT else 0)
        elif kind in (SUM_LEFT, SUM_RIGHT):
            src, dst = share(own, unit, to, kind - SUM_LEFT), slot(arrived, unit, 2 + kind - SUM_LEFT)
        elif kind in (ALL_LEFT, ALL_RIGHT):
            src = dst = shared(unit, me, None)
        else:
            src = dst = shared(unit, right if kind == FAR_LEFT else left, 1 if kind == FAR_LEFT else 0)
        return pltpu.make_async_remote_copy(src_ref=src, dst_ref=dst, send_sem=send.at[u, kind], recv_sem=recv.at[u, kind],
                                            device_id={"dp": to}, device_id_type=MESH)

    def start(u, *kinds):
        for kind in kinds:
            remote(u, kind).start()

    def arrive(u, *kinds):
        for kind in kinds:
            remote(u, kind).wait_recv()

    def each(unit, body):
        down, _, _, size = unit
        many = 64 if down else 16
        blocks = (size // 2 if down else d // (2 * n)) // many
        for which in range(1 if down else 2):
            def one(i, _, which=which):
                rows = pl.ds(pl.multiple_of(i * many, many), many)
                body((rows, slice(None)) if down else (which, rows, slice(None)))
                return 0

            lax.fori_loop(0, blocks, one, 0)

    def forward_sums(u):
        unit = units[u]
        for k, kind, owner in ((0, SUM_LEFT, left), (1, SUM_RIGHT, right)):
            arrive(u, VIA_LEFT + k)
            mine, other = share(own, unit, owner, k), slot(via, unit, k)

            def add(at, mine=mine, other=other):
                mine[at] = (mine[at].astype(F32) + other[at].astype(F32)).astype(BF16)

            each(unit, add)
            start(u, kind)

    def finish(u):
        unit = units[u]
        arrive(u, OWN_LEFT, OWN_RIGHT, SUM_LEFT, SUM_RIGHT)
        for half in range(2):
            mine, out = share(own, unit, me, half), summed(unit, half)
            one, two = slot(arrived, unit, half), slot(arrived, unit, 2 + half)

            def add(at, mine=mine, out=out, one=one, two=two):
                g = (mine[at].astype(F32) + one[at].astype(F32) + two[at].astype(F32)).astype(BF16)
                out[at] = g
                wide = g.astype(F32)
                wide = wide * wide
                total = wide[:, :LANES]
                for k in range(1, wide.shape[1] // LANES):
                    total = total + wide[:, k * LANES : (k + 1) * LANES]
                squares[n] = squares[n] + sum(total[16 * k : 16 * (k + 1)] for k in range(total.shape[0] // 16))

            each(unit, add)

    seconds = {True: (hid1_ref, hid0_ref), False: (dgu1_ref, dgu0_ref)}
    loads = {
        (True, layers - 1): pltpu.make_async_copy(dyt_ref, lefts.at[0], left_sem.at[0]),
        (False, layers - 1): pltpu.make_async_copy(a1t_ref, lefts.at[1], left_sem.at[1]),
        (False, 0): pltpu.make_async_copy(a0t_ref, lefts.at[1], left_sem.at[2]),
    }

    def chunks(u):
        down, _, start_, size = units[u]
        scale = 1 if down else 2
        return scale * start_, scale * size, -(-scale * size // CHUNK)

    def source(u):
        down, layer, _, _ = units[u]
        return seconds[down][layers - 1 - layer]

    def fetch(u, c, parity):
        base, width, _ = chunks(u)
        first = base + jnp.minimum(c * CHUNK, width - CHUNK)
        return pltpu.make_async_copy(source(u).at[:, pl.ds(pl.multiple_of(first, LANES), CHUNK)], rights.at[parity], right_sem.at[parity])

    blocks = ff // LANES
    weight_loads = side_by_side(wg_ref, wu_ref, wgu, layers - 1, weight_sem.at[0])
    weight_loads.append(pltpu.make_async_copy(wd_ref.at[0], wd, weight_sem.at[0, 2 * blocks]))

    def tile_loads(i, parity):
        rows = pl.ds(pl.multiple_of(i * tile, tile), tile)
        copies = [pltpu.make_async_copy(dgu1_ref.at[rows, :], dgu1_in.at[parity], tile_sem.at[0, parity])]
        copies.append(pltpu.make_async_copy(keep_ref.at[rows, :], keep_in.at[parity], tile_sem.at[1, parity]))
        for k, ref in enumerate((h1_ref.at[rows, :], dy_ref.at[0, rows, :])):
            copies.append(pltpu.make_async_copy(ref, small_in.at[k, parity], tile_sem.at[2 + k, parity]))
        return copies

    def tile_store(i, parity):
        rows = pl.ds(pl.multiple_of(i * tile, tile), tile)
        return pltpu.make_async_copy(dgu0_tile.at[parity], dgu0_ref.at[rows, :], back_sem.at[parity])

    def one_tile(i):
        parity = lax.rem(i, 2)
        for copy in tile_loads(i, parity):
            copy.wait()

        @pl.when(i + 1 < tiles)
        def _():
            for copy in tile_loads(i + 1, 1 - parity):
                copy.start()

        @pl.when(i >= 2)
        def _():
            tile_store(i - 2, parity).wait()

        wide, scale, _ = scaled(small_in[0, parity])
        da = by_columns(dgu1_in[parity], wgu[...]).astype(BF16).astype(F32)
        along = jnp.mean(da * wide, -1, keepdims=True)
        dh1 = small_in[1, parity] + (scale * (da - wide * (scale * scale) * along)).astype(BF16)
        lefts[0, :, pl.ds(pl.multiple_of(i * tile, tile), tile)] = dh1.T
        for k, count in grouped(blocks, 4):
            dhid = by_columns(dh1, wd[pl.ds(k * LANES, count * LANES), :]).astype(BF16).astype(F32)
            for j in range(count):
                dh = dhid[:, j * LANES : (j + 1) * LANES]
                for which in range(2):
                    at = lane(2 * (k + j) + which)
                    dgu0_tile[parity, :, at] = (dh * keep_in[parity, :, at]).astype(BF16)
        tile_store(i, parity).start()

    def hand_on(u):
        arrive(u, ALL_LEFT, ALL_RIGHT)
        start(u, FAR_LEFT, FAR_RIGHT)

    def finish_and_send(u):
        finish(u)
        start(u, ALL_LEFT, ALL_RIGHT)

    def tokens_backward(half):
        beside = {1: [(hand_on, 0)], 3: [(forward_sums, half - 1)], 7: [(hand_on, 1)], 10: [(finish_and_send, half - 2)],
                  13: [(finish_and_send, half - 1)]}
        for copy in weight_loads:
            copy.wait()
        loads[(False, 0)].start()

        def one(i, _):
            one_tile(i)
            for when, actions in beside.items():
                @pl.when(i == min(when, tiles - 1))
                def _(actions=actions):
                    for action, u in actions:
                        action(u)
            return 0

        lax.fori_loop(0, tiles, one, 0)
        for i in range(max(0, tiles - 2), tiles):
            tile_store(i, i % 2).wait()

    fetch(0, 0, 0).start()
    loads[(True, layers - 1)].start()
    loads[(False, layers - 1)].start()
    for copy in weight_loads + tile_loads(0, 0):
        copy.start()

    done = 0
    half = len(units) // layers
    for u, unit in enumerate(units):
        down, layer, begin, size = unit
        which = 0 if down else 1
        base, width, count = chunks(u)
        if u == half:
            tokens_backward(half)
            fetch(u, 0, done % 2).start()
        if begin == 0 and (down, layer) in loads:
            loads[(down, layer)].wait()

        def one(c, _, u=u, down=down, layer=layer, which=which, base=base, width=width, count=count, done=done):
            parity = lax.rem(done + c, 2)
            fetch(u, c, parity).wait()

            @pl.when(c + 1 < count)
            def _():
                fetch(u, c + 1, 1 - parity).start()

            if u + 1 < len(units) and u + 1 != half:
                @pl.when(c + 1 == count)
                def _():
                    fetch(u + 1, 0, 1 - parity).start()

            g = jnp.dot(lefts[which], rights[parity], preferred_element_type=F32).astype(BF16)
            first = base + jnp.minimum(c * CHUNK, width - CHUNK)
            if down:
                own_d[layer, pl.ds(pl.multiple_of(first, LANES), CHUNK), :] = g.T
            else:
                for k in range(CHUNK // LANES):
                    at = pl.ds(pl.multiple_of(first // 2 + k // 2 * LANES, LANES), LANES)
                    own_gu[layer, k % 2, :, at] = g[:, k * LANES : (k + 1) * LANES]
            if u % half:
                @pl.when(c == max(0, count - 2))
                def _():
                    forward_sums(u - 1)
            return 0

        lax.fori_loop(0, count, one, 0)
        done += count
        if u == 0:
            squares[n] = jnp.zeros(squares.shape[1:], F32)
            pl.semaphore_wait(barrier, n - 1)
        start(u, VIA_LEFT, VIA_RIGHT, OWN_LEFT, OWN_RIGHT)
        place = u % half
        if u in (half, half + 1):
            hand_on(u - 2)
        if place >= 2:
            finish(u - 2)
            if u < half:
                start(u - 2, ALL_LEFT, ALL_RIGHT)
        if u == half + 2:
            for k in range(half):
                arrive(k, FAR_LEFT, FAR_RIGHT)
            outs = [pltpu.make_async_copy(all_d, gd_out, out_sem.at[0])]
            for k, out in enumerate((gg_out, gu_out)):
                outs.append(pltpu.make_async_copy(all_gu.at[k], out, out_sem.at[1 + k]))
            for out in outs:
                out.start()
    last = len(units) - 1
    parts = []
    many = d // (2 * n)
    for k, part in enumerate((part_a, part_b)):
        for block in range(blocks):
            rows = pl.ds(k * (ff // 2) + block * many, many)
            parts.append(pltpu.make_async_copy(mine_d.at[rows, :], part.at[2, :, lane(block)], out_sem.at[3 + k * (blocks + 1) + block]))
    for part in parts:
        part.start()
    forward_sums(last)
    finish(last - 1)
    finish(last)

    squares[me] = squares[n]
    exchange = [
        pltpu.make_async_remote_copy(src_ref=squares.at[me], dst_ref=squares.at[me], send_sem=sq_send.at[step], recv_sem=sq_recv.at[step],
                                     device_id={"dp": lax.rem(me + step, n)}, device_id_type=MESH)
        for step in range(1, n)
    ]
    for copy in exchange:
        copy.start()
    for k, part in enumerate((part_a, part_b)):
        parts.append(pltpu.make_async_copy(
            mine_gu.at[:, pl.ds(k * many, many), :], part.at[pl.ds(0, 2)], out_sem.at[3 + k * (blocks + 1) + blocks]))
        parts[-1].start()
    for k, (owner, side) in enumerate(((me, 0), (me, 1), (left, 0), (right, 1), (left, 1), (right, 0), (far, 0), (far, 1))):
        places[k] = 2 * owner + side
    for copy in exchange:
        copy.wait_recv()
    total = squares[0]
    for k in range(1, n):
        total = total + squares[k]
    sq_out[...] = total
    for u in range(len(units)):
        for kind in range(10 if u < half else ALL_LEFT):
            remote(u, kind).wait_send()
    for copy in exchange:
        copy.wait_send()
    for out in outs + parts:
        out.wait()


def reduced(n, layers, d, ff, tokens, parts, dy, weights):
    hbm = pl.BlockSpec(memory_space=pl.ANY)
    units = len(units_of(layers, ff))
    tile = min(TILE // 2, tokens)
    dma = pltpu.SemaphoreType.DMA
    part = jax.ShapeDtypeStruct((3, d // (2 * n), ff), BF16)
    return pl.pallas_call(
        functools.partial(reduce_kernel, n),
        out_shape=[
            jax.ShapeDtypeStruct((ff, d), BF16),
            jax.ShapeDtypeStruct((d, ff), BF16),
            jax.ShapeDtypeStruct((d, ff), BF16),
            part,
            part,
            jax.ShapeDtypeStruct((16, LANES), F32),
            jax.ShapeDtypeStruct((2 * n,), jnp.int32),
            jax.ShapeDtypeStruct((tokens, 2 * ff), BF16),
        ],
        in_specs=[hbm] * 12,
        out_specs=[hbm] * 5 + [pl.BlockSpec(memory_space=pltpu.VMEM), pl.BlockSpec(memory_space=pltpu.SMEM), hbm],
        scratch_shapes=[
            pltpu.VMEM((2, d, tokens), BF16),
            pltpu.VMEM((2, tokens, CHUNK), BF16),
            pltpu.VMEM((layers, ff, d), BF16),
            pltpu.VMEM((layers, 2, d, ff), BF16),
            pltpu.VMEM((2, ff // 2, LANES), BF16),
            pltpu.VMEM((2, 2, d // (2 * n), ff), BF16),
            pltpu.VMEM((4, ff // 2, LANES), BF16),
            pltpu.VMEM((4, 2, d // (2 * n), ff), BF16),
            pltpu.VMEM((ff, d), BF16),
            pltpu.VMEM((2, d, ff), BF16),
            pltpu.VMEM((ff, LANES), BF16),
            pltpu.VMEM((2, d // n, ff), BF16),
            pltpu.VMEM((n + 1, 16, LANES), F32),
            pltpu.VMEM((d, 2 * ff), BF16),
            pltpu.VMEM((ff, d), BF16),
            pltpu.VMEM((2, tile, 2 * ff), BF16),
            pltpu.VMEM((2, tile, 2 * ff), F32),
            pltpu.VMEM((2, 2, tile, d), BF16),
            pltpu.VMEM((2, tile, 2 * ff), BF16),
            dma((3,)),
            dma((2,)),
            dma((units, 10)),
            dma((units, 10)),
            dma((n,)),
            dma((n,)),
            dma((3 + 2 * (ff // LANES + 1),)),
            dma((1, 2 * ff // LANES + 1)),
            dma((4, 2)),
            dma((2,)),
        ],
        compiler_params=pltpu.CompilerParams(vmem_limit_bytes=VMEM_LIMIT, collective_id=0, has_side_effects=True),
        cost_estimate=pl.CostEstimate(flops=2 * 9 * tokens * d * ff, bytes_accessed=20 * tokens * ff, transcendentals=tokens * ff),
        name="reduce",
    )(*parts, dy, *weights)


def clip_of(sq_ref, count):
    return jnp.minimum(1.0, 0.5 * lax.rsqrt(jnp.sum(sq_ref[...], keepdims=True) / count + 1e-30))


def update(factor, g, old, new, at):
    w_ref, m_ref, v_ref = old
    g = g.astype(F32) * factor
    w = w_ref[at].astype(F32)
    m = 0.9 * m_ref[at] + 0.1 * g
    v = 0.95 * v_ref[at] + 0.05 * g * g
    step = m * lax.rsqrt(v + 1e-8) + 0.1 * w
    new[0][at] = (w - 0.02 * step).astype(BF16)
    new[1][at] = m
    new[2][at] = v


def whole_kernel(count, sq_ref, *refs):
    factor = clip_of(sq_ref, count)
    for i in range(3):
        g_ref, *old_and_new = refs[i::3]
        update(factor, g_ref[...], old_and_new[:3], old_and_new[3:], (slice(None), slice(None)))


def parts_kernel(count, many, places_ref, sq_ref, *refs):
    parts, refs = refs[:many], refs[many:]
    old, new = refs[:9], refs[18:]
    factor = clip_of(sq_ref, count)
    rows = parts[0].shape[1]
    for k, part in enumerate(parts):
        @pl.when(pl.program_id(0) == k)
        def _(part=part):
            def some(i, _):
                at = pl.ds(pl.multiple_of(i * 16, 16), 16)
                for which in range(2):
                    update(factor, part[which, at, :], old[which::3], new[which::3], (at, slice(None)))
                return 0

            lax.fori_loop(0, rows // 16, some, 0)

            for i in range(part.shape[2] // LANES):
                update(factor, part[2, :, lane(i)], old[2::3], new[2::3], (pl.ds(i * rows, rows), slice(None)))


def adamw_layer(squares, gradients, arrays, layer, blocks):
    count = sum(a.size for a in arrays[:3])
    d, ff = gradients[0].shape
    g_specs = [pl.BlockSpec((d // blocks, ff), lambda i: (i, 0))] * 2 + [pl.BlockSpec((ff // blocks, d), lambda i: (i, 0))]
    specs = [pl.BlockSpec((None, d // blocks, ff), lambda i: (layer, i, 0))] * 2 + [pl.BlockSpec((None, ff // blocks, d), lambda i: (layer, i, 0))]
    return pl.pallas_call(
        functools.partial(whole_kernel, count),
        grid=(blocks,),
        out_shape=[jax.ShapeDtypeStruct(a.shape, a.dtype) for a in arrays],
        in_specs=[pl.BlockSpec(squares.shape, lambda i: (0, 0))] + g_specs + specs * 3,
        out_specs=specs * 3,
        compiler_params=pltpu.CompilerParams(vmem_limit_bytes=VMEM_LIMIT, dimension_semantics=("arbitrary",)),
        cost_estimate=pl.CostEstimate(flops=COST * count // 2, bytes_accessed=11 * count, transcendentals=count),
        name="adamw_layer",
    )(squares, *gradients, *arrays)


def adamw_parts(squares, places, first, parts, arrays, new, layer):
    count = sum(a.size for a in arrays[:3])
    _, rows, ff = parts[0].shape
    many = len(parts)
    by_rows = pl.BlockSpec((None, rows, ff), lambda i, places: (layer, places[first + i], 0))
    by_lanes = pl.BlockSpec((None, ff // 2, LANES), lambda i, places: (layer, places[first + i] % 2, places[first + i] // 2))
    specs = [by_rows, by_rows, by_lanes]
    return pl.pallas_call(
        functools.partial(parts_kernel, count, many),
        grid_spec=pltpu.PrefetchScalarGridSpec(
            num_scalar_prefetch=1,
            grid=(many,),
            in_specs=[pl.BlockSpec(squares.shape, lambda i, places: (0, 0))]
            + [pl.BlockSpec(part.shape, lambda i, places: (0, 0, 0)) for part in parts]
            + specs * 3
            + [pl.BlockSpec(memory_space=pl.ANY)] * 9,
            out_specs=specs * 3,
        ),
        out_shape=[jax.ShapeDtypeStruct(a.shape, a.dtype) for a in arrays],
        input_output_aliases={2 + many + 9 + i: i for i in range(9)},
        compiler_params=pltpu.CompilerParams(vmem_limit_bytes=VMEM_LIMIT, dimension_semantics=("arbitrary",)),
        cost_estimate=pl.CostEstimate(flops=COST * many * 3 * rows * ff, bytes_accessed=22 * many * 3 * rows * ff, transcendentals=many * 3 * rows * ff),
        name="adamw_parts",
    )(places, squares, *parts, *arrays, *new)


COST = 200


def solution(mesh):
    n = mesh.shape["dp"]
    onward = [(i, (i + 1) % n) for i in range(n)]
    back = [(to, i) for i, to in onward]

    def step(x, dy, *arrays):
        weights = arrays[:3]
        layers, ff, d = weights[2].shape
        parts = tokens_pass(x, dy, *weights)
        gd, gg, gu, a, b, squares, places, _ = reduced(n, layers, d, ff, x.shape[1], parts, dy, weights)
        left_a, right_b = lax.ppermute(a, "dp", onward), lax.ppermute(b, "dp", back)
        left_b, right_a = lax.ppermute(b, "dp", onward), lax.ppermute(a, "dp", back)
        new = adamw_layer(squares, (gg, gu, gd), arrays, layers - 1, 4)
        left_a, right_b, *new = lax.optimization_barrier((left_a, right_b, *new))
        far_a, far_b = lax.ppermute(left_a, "dp", onward), lax.ppermute(right_b, "dp", back)
        for first, some in ((0, (a, b, left_a, right_b)), (4, (left_b, right_a, far_a, far_b))):
            new = adamw_parts(squares, places, first, some, arrays, new, 0)
        return tuple(new)

    return jax.shard_map(
        step,
        mesh=mesh,
        in_specs=(P(("rep", "dp"), None, None),) * 2 + (P(None, None, None),) * 9,
        out_specs=(P("rep", None, None),) * 9,
        check_vma=False,
    )
```

```python
import functools

import jax
import jax.numpy as jnp
from jax import lax
from jax.experimental import pallas as pl
from jax.experimental.pallas import tpu as pltpu
from jax.sharding import PartitionSpec as P

F32, BF16 = jnp.float32, jnp.bfloat16
MESH = pl.DeviceIdType.MESH
LANES = 128
VMEM_LIMIT = 67043328
TILE = 512
CHUNK = 4 * LANES
MOST_ROWS = 192
RUNS = 4


def by_columns(a, b):
    return lax.dot_general(a, b, (((1,), (1,)), ((), ())), preferred_element_type=F32)


def scaled(h):
    wide = h.astype(F32)
    scale = lax.rsqrt(jnp.mean(wide * wide, -1, keepdims=True) + 1e-6)
    return wide, scale, (wide * scale).astype(BF16)


def lane(k):
    return pl.ds(k * LANES, LANES)


def side_by_side(wg_ref, wu_ref, wgu, n, sems):
    return [
        pltpu.make_async_copy(ref.at[n, :, lane(k)], wgu.at[:, lane(2 * k + which)], sems.at[2 * k + which])
        for k in range(wg_ref.shape[-1] // LANES)
        for which, ref in enumerate((wg_ref, wu_ref))
    ]


def grouped(blocks, many):
    return [(k, min(many, blocks - k)) for k in range(0, blocks, many)]


def tokens_kernel(x_ref, dy_ref, wg_ref, wu_ref, wd_ref, dyt_ref, a1t_ref, a0t_ref, h1_ref, hid1_ref, dgu1_ref, hid0_ref,
                  keep_ref, wgu, wd, sems, *, many):
    layers, ff, _ = wd.shape
    blocks = ff // LANES

    first = pl.program_id(0) == 0
    loads = [[*side_by_side(wg_ref, wu_ref, wgu.at[n], n, sems.at[n]), pltpu.make_async_copy(wd_ref.at[n], wd.at[n], sems.at[n, 2 * blocks])]
             for n in range(layers)]

    @pl.when(first)
    def _():
        for copies in loads:
            for copy in copies:
                copy.start()
        for copy in loads[0]:
            copy.wait()

    groups = grouped(blocks, many)
    h0 = x_ref[...]
    _, _, a0 = scaled(h0)
    a0t_ref[...] = a0.T
    for k, count in groups:
        gu = jnp.dot(a0, wgu[0, :, pl.ds(2 * k * LANES, 2 * count * LANES)], preferred_element_type=F32)
        for i in range(count):
            g, u = (gu[:, (2 * i + j) * LANES : (2 * i + j + 1) * LANES] for j in range(2))
            s = 0.5 * jnp.tanh(0.5 * g) + 0.5
            silu = g * s
            hid0_ref[:, lane(k + i)] = (silu * u).astype(BF16)
            keep_ref[:, lane(2 * (k + i))] = (s + silu * (1.0 - s)) * u
            keep_ref[:, lane(2 * (k + i) + 1)] = silu
    h1 = h0 + jnp.dot(hid0_ref[...], wd[0], preferred_element_type=F32).astype(BF16)
    h1_ref[...] = h1
    _, _, a1 = scaled(h1)
    a1t_ref[...] = a1.T
    dy = dy_ref[...]
    dyt_ref[...] = dy.T

    @pl.when(first)
    def _():
        for copy in loads[1]:
            copy.wait()

    for k, count in groups:
        gu = jnp.dot(a1, wgu[1, :, pl.ds(2 * k * LANES, 2 * count * LANES)], preferred_element_type=F32)
        dhid = by_columns(dy, wd[1, pl.ds(k * LANES, count * LANES), :]).astype(BF16).astype(F32)
        for i in range(count):
            g, u = (gu[:, (2 * i + j) * LANES : (2 * i + j + 1) * LANES] for j in range(2))
            dh = dhid[:, i * LANES : (i + 1) * LANES]
            s = 0.5 * jnp.tanh(0.5 * g) + 0.5
            silu = g * s
            hid1_ref[:, lane(k + i)] = (silu * u).astype(BF16)
            dgu1_ref[:, lane(2 * (k + i))] = (dh * u * (s + silu * (1.0 - s))).astype(BF16)
            dgu1_ref[:, lane(2 * (k + i) + 1)] = (dh * silu).astype(BF16)


def tokens_pass(x, dy, wg, wu, wd):
    _, tokens, d = x.shape
    layers, ff, _ = wd.shape
    tile = min(TILE, tokens)
    lead = pl.BlockSpec((None, tile, d), lambda i: (0, i, 0))
    hbm = pl.BlockSpec(memory_space=pl.ANY)
    turned = pl.BlockSpec((d, tile), lambda i: (0, i))
    widths = (d, ff, 2 * ff, ff, 2 * ff)
    return pl.pallas_call(
        functools.partial(tokens_kernel, many=2),
        grid=(tokens // tile,),
        out_shape=[jax.ShapeDtypeStruct((d, tokens), BF16)] * 3 + [
            jax.ShapeDtypeStruct((tokens, n), F32 if k == 4 else BF16) for k, n in enumerate(widths)
        ],
        in_specs=[lead, lead, hbm, hbm, hbm],
        out_specs=[turned] * 3 + [pl.BlockSpec((tile, n), lambda i: (i, 0)) for n in widths],
        scratch_shapes=[
            pltpu.VMEM((layers, d, 2 * ff), BF16),
            pltpu.VMEM((layers, ff, d), BF16),
            pltpu.SemaphoreType.DMA((layers, 2 * ff // LANES + 1)),
        ],
        compiler_params=pltpu.CompilerParams(vmem_limit_bytes=VMEM_LIMIT, dimension_semantics=("arbitrary",)),
        cost_estimate=pl.CostEstimate(flops=2 * 6 * tokens * d * ff, bytes_accessed=10 * tokens * ff, transcendentals=2 * tokens * ff),
        name="tokens",
    )(x, dy, wg, wu, wd)


(VIA_LEFT, VIA_RIGHT, OWN_LEFT, OWN_RIGHT, SUM_LEFT, SUM_RIGHT, ALL_LEFT, ALL_RIGHT, FAR_LEFT, FAR_RIGHT) = range(10)


def units_of(layers, ff):
    cuts = {True: CHUNK, False: (ff // CHUNK) * CHUNK // 2}
    return [
        (down, n, start, size)
        for n in reversed(range(layers))
        for down, cut in cuts.items()
        for start, size in ((0, cut), (cut, ff - cut))
    ]


def reduce_kernel(n, dyt_ref, a1t_ref, a0t_ref, h1_ref, hid1_ref, dgu1_ref, hid0_ref, keep_ref, dy_ref, wg_ref, wu_ref, wd_ref,
                  gd_out, gg_out, gu_out, part_a, part_b, sq_out, places, dgu0_ref,
                  lefts, rights, own_d, own_gu, via_d, via_gu, in_d, in_gu, all_d, all_gu, mine_d, mine_gu, squares,
                  wgu, wd, dgu1_in, keep_in, small_in, dgu0_tile,
                  left_sem, right_sem, send, recv, sq_send, sq_recv, out_sem, weight_sem, tile_sem, back_sem, first_sem):
    layers, ff, d = own_d.shape
    tile = dgu0_tile.shape[1]
    tiles = h1_ref.shape[0] // tile
    units = units_of(layers, ff)
    me = lax.axis_index("dp")
    right, left, far = lax.rem(me + 1, n), lax.rem(me + n - 1, n), lax.rem(me + n // 2, n)

    barrier = pltpu.get_barrier_semaphore()
    for step in range(1, n):
        pl.semaphore_signal(barrier, inc=1, device_id={"dp": lax.rem(me + step, n)}, device_id_type=MESH)

    def within(unit, owner, half):
        down, _, start, size = unit
        if down:
            rows = pl.ds(start, size) if half is None else pl.ds(start + half * (size // 2), size // 2)
            return rows, pl.ds(pl.multiple_of(owner * LANES, LANES), LANES)
        rows = d // n
        first = owner * rows
        if half is not None:
            rows = rows // 2
            first = first + half * rows
        return slice(None), pl.ds(pl.multiple_of(first, 16), rows), pl.ds(start, size)

    def share(ref, unit, owner, half):
        return ref[0 if unit[0] else 1].at[(unit[1], *within(unit, owner, half))]

    def shared(unit, owner, half):
        return whole[0 if unit[0] else 1].at[within(unit, owner, half)]

    def slot(ref, unit, k):
        down, layer, start, size = unit
        if down:
            return ref[0].at[k, pl.ds(start // 2, size // 2), :]
        return ref[1].at[k, :, :, pl.ds(start, size)]

    def summed(unit, half):
        if unit[1]:
            return shared(unit, me, half)
        return (mine_d if unit[0] else mine_gu).at[within(unit, 0, half)]

    own, via, arrived, whole = (own_d, own_gu), (via_d, via_gu), (in_d, in_gu), (all_d, all_gu)

    def remote(u, kind):
        unit = units[u]
        to = left if kind % 2 == 0 else right
        if kind in (VIA_LEFT, VIA_RIGHT):
            src, dst = share(own, unit, far, kind - VIA_LEFT), slot(via, unit, kind - VIA_LEFT)
        elif kind in (OWN_LEFT, OWN_RIGHT):
            src, dst = share(own, unit, to, 1 if kind == OWN_LEFT else 0), slot(arrived, unit, 1 if kind == OWN_LEFT else 0)
        elif kind in (SUM_LEFT, SUM_RIGHT):
            src, dst = share(own, unit, to, kind - SUM_LEFT), slot(arrived, unit, 2 + kind - SUM_LEFT)
        elif kind in (ALL_LEFT, ALL_RIGHT):
            src = dst = shared(unit, me, None)
        else:
            src = dst = shared(unit, right if kind == FAR_LEFT else left, 1 if kind == FAR_LEFT else 0)
        return pltpu.make_async_remote_copy(src_ref=src, dst_ref=dst, send_sem=send.at[u, kind], recv_sem=recv.at[u, kind],
                                            device_id={"dp": to}, device_id_type=MESH)

    def start(u, *kinds):
        for kind in kinds:
            remote(u, kind).start()

    def arrive(u, *kinds):
        for kind in kinds:
            remote(u, kind).wait_recv()

    def each(unit, body):
        down, _, _, size = unit
        rows = size // 2 if down else d // (2 * n)
        many = max(m for m in range(16, MOST_ROWS + 16, 16) if rows % m == 0) if down else rows
        blocks = rows // many
        for which in range(1 if down else 2):
            def one(i, _, which=which):
                rows = pl.ds(pl.multiple_of(i * many, many), many)
                body((rows, slice(None)) if down else (which, rows, slice(None)))
                return 0

            lax.fori_loop(0, blocks, one, 0)

    def forward_sums(u):
        unit = units[u]
        for k, kind, owner in ((0, SUM_LEFT, left), (1, SUM_RIGHT, right)):
            arrive(u, VIA_LEFT + k)
            mine, other = share(own, unit, owner, k), slot(via, unit, k)

            def add(at, mine=mine, other=other):
                mine[at] = (mine[at].astype(F32) + other[at].astype(F32)).astype(BF16)

            each(unit, add)
            start(u, kind)

    def finish(u):
        unit = units[u]
        arrive(u, OWN_LEFT, OWN_RIGHT, SUM_LEFT, SUM_RIGHT)
        for half in range(2):
            mine, out = share(own, unit, me, half), summed(unit, half)
            one, two = slot(arrived, unit, half), slot(arrived, unit, 2 + half)

            def add(at, mine=mine, out=out, one=one, two=two):
                g = (mine[at].astype(F32) + one[at].astype(F32) + two[at].astype(F32)).astype(BF16)
                out[at] = g
                wide = g.astype(F32)
                wide = wide * wide
                total = wide[:, :LANES]
                for k in range(1, wide.shape[1] // LANES):
                    total = total + wide[:, k * LANES : (k + 1) * LANES]
                squares[n] = squares[n] + sum(total[16 * k : 16 * (k + 1)] for k in range(total.shape[0] // 16))

            each(unit, add)

    seconds = {True: (hid1_ref, hid0_ref), False: (dgu1_ref, dgu0_ref)}
    loads = {
        (False, layers - 1): pltpu.make_async_copy(a1t_ref, lefts.at[1], left_sem.at[1]),
        (False, 0): pltpu.make_async_copy(a0t_ref, lefts.at[1], left_sem.at[2]),
    }

    def chunks(u):
        down, _, start_, size = units[u]
        scale = 1 if down else 2
        return scale * start_, scale * size, -(-scale * size // CHUNK)

    def source(u):
        down, layer, _, _ = units[u]
        return seconds[down][layers - 1 - layer]

    def fetch(u, c, parity):
        base, width, _ = chunks(u)
        first = base + jnp.minimum(c * CHUNK, width - CHUNK)
        return pltpu.make_async_copy(source(u).at[:, pl.ds(pl.multiple_of(first, LANES), CHUNK)], rights.at[parity], right_sem.at[parity])

    blocks = ff // LANES
    weight_loads = side_by_side(wg_ref, wu_ref, wgu, layers - 1, weight_sem.at[0])
    weight_loads.append(pltpu.make_async_copy(wd_ref.at[0], wd, weight_sem.at[0, 2 * blocks]))

    def tile_loads(i, parity):
        rows = pl.ds(pl.multiple_of(i * tile, tile), tile)
        copies = [pltpu.make_async_copy(dgu1_ref.at[rows, :], dgu1_in.at[parity], tile_sem.at[0, parity])]
        copies.append(pltpu.make_async_copy(keep_ref.at[rows, :], keep_in.at[parity], tile_sem.at[1, parity]))
        for k, ref in enumerate((h1_ref.at[rows, :], dy_ref.at[0, rows, :])):
            copies.append(pltpu.make_async_copy(ref, small_in.at[k, parity], tile_sem.at[2 + k, parity]))
        return copies

    def tile_store(i, parity):
        rows = pl.ds(pl.multiple_of(i * tile, tile), tile)
        return pltpu.make_async_copy(dgu0_tile.at[parity], dgu0_ref.at[rows, :], back_sem.at[parity])

    def one_tile(i):
        parity = lax.rem(i, 2)
        for copy in tile_loads(i, parity):
            copy.wait()

        @pl.when(i + 1 < tiles)
        def _():
            for copy in tile_loads(i + 1, 1 - parity):
                copy.start()

        @pl.when(i >= 2)
        def _():
            tile_store(i - 2, parity).wait()

        wide, scale, _ = scaled(small_in[0, parity])
        da = by_columns(dgu1_in[parity], wgu[...]).astype(BF16).astype(F32)
        along = jnp.mean(da * wide, -1, keepdims=True)
        dh1 = small_in[1, parity] + (scale * (da - wide * (scale * scale) * along)).astype(BF16)
        lefts[0, :, pl.ds(pl.multiple_of(i * tile, tile), tile)] = dh1.T
        for k, count in grouped(blocks, 4):
            dhid = by_columns(dh1, wd[pl.ds(k * LANES, count * LANES), :]).astype(BF16).astype(F32)
            for j in range(count):
                dh = dhid[:, j * LANES : (j + 1) * LANES]
                for which in range(2):
                    at = lane(2 * (k + j) + which)
                    dgu0_tile[parity, :, at] = (dh * keep_in[parity, :, at]).astype(BF16)
        tile_store(i, parity).start()

    def hand_on(u):
        arrive(u, ALL_LEFT, ALL_RIGHT)
        start(u, FAR_LEFT, FAR_RIGHT)

    def finish_and_send(u):
        finish(u)
        start(u, ALL_LEFT, ALL_RIGHT)

    def tokens_backward(half):
        beside = {1: [(hand_on, 0)], 3: [(forward_sums, half - 1)], 7: [(hand_on, 1)], 10: [(finish_and_send, half - 2)],
                  13: [(finish_and_send, half - 1)]}
        for copy in weight_loads:
            copy.wait()
        loads[(False, 0)].start()

        def one(i, _):
            one_tile(i)
            for when, actions in beside.items():
                @pl.when(i == min(when, tiles - 1))
                def _(actions=actions):
                    for action, u in actions:
                        action(u)
            return 0

        lax.fori_loop(0, tiles, one, 0)
        for i in range(max(0, tiles - 2), tiles):
            tile_store(i, i % 2).wait()

    runs = [pl.ds(k * (tiles * tile // RUNS), tiles * tile // RUNS) for k in range(RUNS)]
    first_loads = [
        (pltpu.make_async_copy(dyt_ref.at[:, run], lefts.at[0, :, run], first_sem.at[0, k]),
         pltpu.make_async_copy(hid1_ref.at[run, pl.ds(0, CHUNK)], rights.at[0, run, :], first_sem.at[1, k]))
        for k, run in enumerate(runs)
    ]
    for pair in first_loads:
        for copy in pair:
            copy.start()

    done = 0
    half = len(units) // layers
    for u, unit in enumerate(units):
        down, layer, begin, size = unit
        which = 0 if down else 1
        base, width, count = chunks(u)
        if u == half:
            tokens_backward(half)
            fetch(u, 0, done % 2).start()
        if begin == 0 and (down, layer) in loads:
            loads[(down, layer)].wait()

        def one(c, _, u=u, down=down, layer=layer, which=which, base=base, width=width, count=count, done=done):
            parity = lax.rem(done + c, 2)
            fetch(u, c, parity).wait()

            @pl.when(c + 1 < count)
            def _():
                fetch(u, c + 1, 1 - parity).start()

            if u + 1 < len(units) and u + 1 != half:
                @pl.when(c + 1 == count)
                def _():
                    fetch(u + 1, 0, 1 - parity).start()

            g = jnp.dot(lefts[which], rights[parity], preferred_element_type=F32).astype(BF16)
            first = base + jnp.minimum(c * CHUNK, width - CHUNK)
            if down:
                own_d[layer, pl.ds(pl.multiple_of(first, LANES), CHUNK), :] = g.T
            else:
                for k in range(CHUNK // LANES):
                    at = pl.ds(pl.multiple_of(first // 2 + k // 2 * LANES, LANES), LANES)
                    own_gu[layer, k % 2, :, at] = g[:, k * LANES : (k + 1) * LANES]
            if u % half:
                @pl.when(c == max(0, count - 2))
                def _():
                    forward_sums(u - 1)
            return 0

        if u == 0:
            total = None
            for pair, run in zip(first_loads, runs, strict=True):
                for copy in pair:
                    copy.wait()
                term = jnp.dot(lefts[0, :, run], rights[0, run, :], preferred_element_type=F32)
                total = term if total is None else total + term
            fetch(1, 0, 1).start()
            own_d[layer, pl.ds(0, CHUNK), :] = total.astype(BF16).T
            loads[(False, layers - 1)].start()
        else:
            lax.fori_loop(0, count, one, 0)
        if u == 2:
            for copy in weight_loads + tile_loads(0, 0):
                copy.start()
        done += count
        if u == 0:
            squares[n] = jnp.zeros(squares.shape[1:], F32)
            pl.semaphore_wait(barrier, n - 1)
        start(u, VIA_LEFT, VIA_RIGHT, OWN_LEFT, OWN_RIGHT)
        place = u % half
        if u in (half, half + 1):
            hand_on(u - 2)
        if place >= 2:
            finish(u - 2)
            if u < half:
                start(u - 2, ALL_LEFT, ALL_RIGHT)
        if u == half + 2:
            for k in range(half):
                arrive(k, FAR_LEFT, FAR_RIGHT)
            outs = [pltpu.make_async_copy(all_d, gd_out, out_sem.at[0])]
            for k, out in enumerate((gg_out, gu_out)):
                outs.append(pltpu.make_async_copy(all_gu.at[k], out, out_sem.at[1 + k]))
            for out in outs:
                out.start()
    last = len(units) - 1
    parts = []
    many = d // (2 * n)
    for k, part in enumerate((part_a, part_b)):
        for block in range(blocks):
            rows = pl.ds(k * (ff // 2) + block * many, many)
            parts.append(pltpu.make_async_copy(mine_d.at[rows, :], part.at[2, :, lane(block)], out_sem.at[3 + k * (blocks + 1) + block]))
    for part in parts:
        part.start()
    forward_sums(last)
    finish(last - 1)
    finish(last)

    squares[me] = squares[n]
    exchange = [
        pltpu.make_async_remote_copy(src_ref=squares.at[me], dst_ref=squares.at[me], send_sem=sq_send.at[step], recv_sem=sq_recv.at[step],
                                     device_id={"dp": lax.rem(me + step, n)}, device_id_type=MESH)
        for step in range(1, n)
    ]
    for copy in exchange:
        copy.start()
    for k, part in enumerate((part_a, part_b)):
        parts.append(pltpu.make_async_copy(
            mine_gu.at[:, pl.ds(k * many, many), :], part.at[pl.ds(0, 2)], out_sem.at[3 + k * (blocks + 1) + blocks]))
        parts[-1].start()
    for k, owner in enumerate((me, left, right, far)):
        places[2 * k] = 2 * owner
        places[2 * k + 1] = 2 * owner + 1
    for copy in exchange:
        copy.wait_recv()
    total = squares[0]
    for k in range(1, n):
        total = total + squares[k]
    sq_out[...] = total
    for u in range(len(units)):
        for kind in range(10 if u < half else ALL_LEFT):
            remote(u, kind).wait_send()
    for copy in exchange:
        copy.wait_send()
    for out in outs + parts:
        out.wait()


def reduced(n, layers, d, ff, tokens, parts, dy, weights):
    hbm = pl.BlockSpec(memory_space=pl.ANY)
    units = len(units_of(layers, ff))
    tile = min(TILE // 2, tokens)
    dma = pltpu.SemaphoreType.DMA
    part = jax.ShapeDtypeStruct((3, d // (2 * n), ff), BF16)
    return pl.pallas_call(
        functools.partial(reduce_kernel, n),
        out_shape=[
            jax.ShapeDtypeStruct((ff, d), BF16),
            jax.ShapeDtypeStruct((d, ff), BF16),
            jax.ShapeDtypeStruct((d, ff), BF16),
            part,
            part,
            jax.ShapeDtypeStruct((16, LANES), F32),
            jax.ShapeDtypeStruct((2 * n,), jnp.int32),
            jax.ShapeDtypeStruct((tokens, 2 * ff), BF16),
        ],
        in_specs=[hbm] * 12,
        out_specs=[hbm] * 5 + [pl.BlockSpec(memory_space=pltpu.VMEM), pl.BlockSpec(memory_space=pltpu.SMEM), hbm],
        scratch_shapes=[
            pltpu.VMEM((2, d, tokens), BF16),
            pltpu.VMEM((2, tokens, CHUNK), BF16),
            pltpu.VMEM((layers, ff, d), BF16),
            pltpu.VMEM((layers, 2, d, ff), BF16),
            pltpu.VMEM((2, ff // 2, LANES), BF16),
            pltpu.VMEM((2, 2, d // (2 * n), ff), BF16),
            pltpu.VMEM((4, ff // 2, LANES), BF16),
            pltpu.VMEM((4, 2, d // (2 * n), ff), BF16),
            pltpu.VMEM((ff, d), BF16),
            pltpu.VMEM((2, d, ff), BF16),
            pltpu.VMEM((ff, LANES), BF16),
            pltpu.VMEM((2, d // n, ff), BF16),
            pltpu.VMEM((n + 1, 16, LANES), F32),
            pltpu.VMEM((d, 2 * ff), BF16),
            pltpu.VMEM((ff, d), BF16),
            pltpu.VMEM((2, tile, 2 * ff), BF16),
            pltpu.VMEM((2, tile, 2 * ff), F32),
            pltpu.VMEM((2, 2, tile, d), BF16),
            pltpu.VMEM((2, tile, 2 * ff), BF16),
            dma((3,)),
            dma((2,)),
            dma((units, 10)),
            dma((units, 10)),
            dma((n,)),
            dma((n,)),
            dma((3 + 2 * (ff // LANES + 1),)),
            dma((1, 2 * ff // LANES + 1)),
            dma((4, 2)),
            dma((2,)),
            dma((2, RUNS)),
        ],
        compiler_params=pltpu.CompilerParams(vmem_limit_bytes=VMEM_LIMIT, collective_id=0, has_side_effects=True),
        cost_estimate=pl.CostEstimate(flops=2 * 9 * tokens * d * ff, bytes_accessed=20 * tokens * ff, transcendentals=tokens * ff),
        name="reduce",
    )(*parts, dy, *weights)


def clip_of(sq_ref, count):
    return jnp.minimum(1.0, 0.5 * lax.rsqrt(jnp.sum(sq_ref[...], keepdims=True) / count + 1e-30))


def update(factor, g, old, new, at):
    w_ref, m_ref, v_ref = old
    g = g.astype(F32) * factor
    w = w_ref[at].astype(F32)
    m = 0.9 * m_ref[at] + 0.1 * g
    v = 0.95 * v_ref[at] + 0.05 * g * g
    step = m * lax.rsqrt(v + 1e-8) + 0.1 * w
    new[0][at] = (w - 0.02 * step).astype(BF16)
    new[1][at] = m
    new[2][at] = v


def whole_kernel(count, sq_ref, *refs):
    factor = clip_of(sq_ref, count)
    for i in range(3):
        g_ref, *old_and_new = refs[i::3]
        update(factor, g_ref[...], old_and_new[:3], old_and_new[3:], (slice(None), slice(None)))


def parts_kernel(count, many, places_ref, sq_ref, *refs):
    parts, refs = refs[:many], refs[many:]
    old, new = refs[:9], refs[18:]
    factor = clip_of(sq_ref, count)
    rows = parts[0].shape[1]
    for k, part in enumerate(parts):
        @pl.when(pl.program_id(0) == k)
        def _(part=part):
            def some(i, _):
                at = pl.ds(pl.multiple_of(i * 16, 16), 16)
                for which in range(2):
                    update(factor, part[which, at, :], old[which::3], new[which::3], (at, slice(None)))
                return 0

            lax.fori_loop(0, rows // 16, some, 0)

            for i in range(part.shape[2] // LANES):
                update(factor, part[2, :, lane(i)], old[2::3], new[2::3], (pl.ds(i * rows, rows), slice(None)))


def adamw_layer(squares, gradients, arrays, layer, blocks):
    count = sum(a.size for a in arrays[:3])
    d, ff = gradients[0].shape
    g_specs = [pl.BlockSpec((d // blocks, ff), lambda i: (i, 0))] * 2 + [pl.BlockSpec((ff // blocks, d), lambda i: (i, 0))]
    specs = [pl.BlockSpec((None, d // blocks, ff), lambda i: (layer, i, 0))] * 2 + [pl.BlockSpec((None, ff // blocks, d), lambda i: (layer, i, 0))]
    return pl.pallas_call(
        functools.partial(whole_kernel, count),
        grid=(blocks,),
        out_shape=[jax.ShapeDtypeStruct(a.shape, a.dtype) for a in arrays],
        in_specs=[pl.BlockSpec(squares.shape, lambda i: (0, 0))] + g_specs + specs * 3,
        out_specs=specs * 3,
        compiler_params=pltpu.CompilerParams(vmem_limit_bytes=VMEM_LIMIT, dimension_semantics=("arbitrary",)),
        cost_estimate=pl.CostEstimate(flops=COST * count // 2, bytes_accessed=11 * count, transcendentals=count),
        name="adamw_layer",
    )(squares, *gradients, *arrays)


def adamw_parts(squares, places, first, parts, arrays, new, layer):
    count = sum(a.size for a in arrays[:3])
    _, rows, ff = parts[0].shape
    many = len(parts)
    by_rows = pl.BlockSpec((None, rows, ff), lambda i, places: (layer, places[first + i], 0))
    by_lanes = pl.BlockSpec((None, ff // 2, LANES), lambda i, places: (layer, places[first + i] % 2, places[first + i] // 2))
    specs = [by_rows, by_rows, by_lanes]
    return pl.pallas_call(
        functools.partial(parts_kernel, count, many),
        grid_spec=pltpu.PrefetchScalarGridSpec(
            num_scalar_prefetch=1,
            grid=(many,),
            in_specs=[pl.BlockSpec(squares.shape, lambda i, places: (0, 0))]
            + [pl.BlockSpec(part.shape, lambda i, places: (0, 0, 0)) for part in parts]
            + specs * 3
            + [pl.BlockSpec(memory_space=pl.ANY)] * 9,
            out_specs=specs * 3,
        ),
        out_shape=[jax.ShapeDtypeStruct(a.shape, a.dtype) for a in arrays],
        input_output_aliases={2 + many + 9 + i: i for i in range(9)},
        compiler_params=pltpu.CompilerParams(vmem_limit_bytes=VMEM_LIMIT, dimension_semantics=("arbitrary",)),
        cost_estimate=pl.CostEstimate(flops=COST * many * 3 * rows * ff, bytes_accessed=22 * many * 3 * rows * ff, transcendentals=many * 3 * rows * ff),
        name="adamw_parts",
    )(places, squares, *parts, *arrays, *new)


COST = 200


def solution(mesh):
    n = mesh.shape["dp"]
    onward = [(i, (i + 1) % n) for i in range(n)]
    back = [(to, i) for i, to in onward]

    def step(x, dy, *arrays):
        weights = arrays[:3]
        layers, ff, d = weights[2].shape
        parts = tokens_pass(x, dy, *weights)
        gd, gg, gu, a, b, squares, places, _ = reduced(n, layers, d, ff, x.shape[1], parts, dy, weights)
        left_a, right_b = lax.ppermute(a, "dp", onward), lax.ppermute(b, "dp", back)
        left_b, right_a = lax.ppermute(b, "dp", onward), lax.ppermute(a, "dp", back)
        new = adamw_layer(squares, (gg, gu, gd), arrays, layers - 1, 4)
        left_a, right_b, *new = lax.optimization_barrier((left_a, right_b, *new))
        far_a, far_b = lax.ppermute(left_a, "dp", onward), lax.ppermute(right_b, "dp", back)
        for first, some in ((0, (a, b)), (2, (left_a, left_b, right_a, right_b)), (6, (far_a, far_b))):
            new = adamw_parts(squares, places, first, some, arrays, new, 0)
        return tuple(new)

    return jax.shard_map(
        step,
        mesh=mesh,
        in_specs=(P(("rep", "dp"), None, None),) * 2 + (P(None, None, None),) * 9,
        out_specs=(P("rep", None, None),) * 9,
        check_vma=False,
    )
```
